32 devices in a mesh: rep: 1 (over z), dp: 32 (over x, y, core).
Axes of the slice: x: 4, y: 4, z: 1, core: 2. Of those that a mesh axis runs over, the one named last changes fastest.
The devices are a block of a 4x4x8 slice.
Arguments:
- x: bfloat16 [32, 2048, 640], P(('rep', 'dp'))
- dy: bfloat16 [32, 2048, 640], P(('rep', 'dp'))
- w_gate: bfloat16 [2, 640, 3200], replicated
- w_up: bfloat16 [2, 640, 3200], replicated
- w_down: bfloat16 [2, 3200, 640], replicated
- m_w_gate: float32 [2, 640, 3200], replicated
- m_w_up: float32 [2, 640, 3200], replicated
- m_w_down: float32 [2, 3200, 640], replicated
- v_w_gate: float32 [2, 640, 3200], replicated
- v_w_up: float32 [2, 640, 3200], replicated
- v_w_down: float32 [2, 3200, 640], replicated
Outputs:
- output 1: bfloat16 [2, 640, 3200], P('rep')
- output 2: bfloat16 [2, 640, 3200], P('rep')
- output 3: bfloat16 [2, 3200, 640], P('rep')
- output 4: float32 [2, 640, 3200], P('rep')
- output 5: float32 [2, 640, 3200], P('rep')
- output 6: float32 [2, 3200, 640], P('rep')
- output 7: float32 [2, 640, 3200], P('rep')
- output 8: float32 [2, 640, 3200], P('rep')
- output 9: float32 [2, 3200, 640], P('rep')
All inputs are finite; a program needn't handle non-finite values.
Results may differ from the reference program's by a relative error of at most 0.022.
Values are sent between devices in bfloat16 or wider.
A program may use at most 768 MiB of HBM per device.

```python
import jax
import jax.numpy as jnp
from jax import lax

SEQUENCES = 32
TOKENS = 2048
D = 640
FF = 3200
LAYERS = 2
NAMES = ("w_gate", "w_up", "w_down")
SHAPES = {"w_gate": (LAYERS, D, FF), "w_up": (LAYERS, D, FF), "w_down": (LAYERS, FF, D)}


def bump(key, n, height):
    away = (jnp.arange(n, dtype=jnp.int32) - jax.random.randint(key, (), 0, n, jnp.int32)) % n
    return jnp.where(away < n // 8, height, 1.0)


def together(key, own, strength):
    shared = jax.random.normal(key, own.shape[1:], jnp.float32)
    return (own + strength * shared) * lax.rsqrt(1 + strength * strength)


def setup_inputs(seed: int = 0, part: int = 0) -> dict:
    kx, kdy, ka, kb, kz, kf, kh, kl, *keys = jax.random.split(jax.random.key(seed), 8 + 3 * len(NAMES))
    kx, kdy, ka, kb = (jax.random.fold_in(k, part) for k in (kx, kdy, ka, kb))
    kw, km, kv = (keys[i::3] for i in range(3))
    shape = (SEQUENCES, TOKENS, D)
    much_x, much_dy = jax.random.uniform(kz, (2,), jnp.float32, 0.0, 1.0)
    loud = 2.0 ** jax.random.uniform(jax.random.fold_in(kz, 1), (), jnp.float32, -1.0, 2.0)
    layers = 2.0 ** jax.random.uniform(kl, (LAYERS, 1, 1), jnp.float32, -1.0, 1.0)
    x = together(ka, jax.random.normal(kx, shape, jnp.float32), much_x) * bump(kf, D, 4.0)
    dy = together(kb, jax.random.normal(kdy, shape, jnp.float32), much_dy)
    drawn = {"x": x.astype(jnp.bfloat16), "dy": (loud * dy * (SEQUENCES * TOKENS) ** -0.5).astype(jnp.bfloat16)}
    for key, name in zip(kw, NAMES, strict=True):
        w = jax.random.normal(key, SHAPES[name], jnp.float32) * SHAPES[name][1] ** -0.5
        drawn[name] = (w * {"w_gate": 1.0, "w_up": bump(kh, FF, 4.0), "w_down": layers}[name]).astype(jnp.bfloat16)
    for key, name in zip(km, NAMES, strict=True):
        drawn[f"m_{name}"] = 0.1 * jax.random.normal(key, SHAPES[name], jnp.float32)
    for key, name in zip(kv, NAMES, strict=True):
        drawn[f"v_{name}"] = jax.random.uniform(key, SHAPES[name], jnp.float32, 0.005, 0.015)
    return drawn


def matmul(a, w):
    return jnp.dot(a, w, preferred_element_type=jnp.float32).astype(jnp.bfloat16)


def normed(h):
    wide = h.astype(jnp.float32)
    scale = lax.rsqrt(jnp.mean(wide**2, -1, keepdims=True) + 1e-6)
    return (wide * scale).astype(jnp.bfloat16)


def layer(h, w):
    a = normed(h)
    gate = jnp.dot(a, w["w_gate"], preferred_element_type=jnp.float32)
    up = jnp.dot(a, w["w_up"], preferred_element_type=jnp.float32)
    return h + matmul((jax.nn.silu(gate) * up).astype(jnp.bfloat16), w["w_down"])


def adamw(w, m, v, g):
    m = 0.9 * m + 0.1 * g
    v = 0.95 * v + 0.05 * g * g
    step = m * lax.rsqrt(v + 1e-8) + 0.1 * w
    return (w - 0.02 * step).astype(jnp.bfloat16), m, v


def stack(weights, h):
    return lax.scan(lambda h, w: (layer(h, w), None), h, weights)[0]


def reference(x, dy, w_gate, w_up, w_down, m_w_gate, m_w_up, m_w_down, v_w_gate, v_w_up, v_w_down):
    weights = dict(zip(NAMES, (w_gate, w_up, w_down), strict=True))

    def take(so_far, sequence):
        h, by_y = sequence
        _, back = jax.vjp(lambda w: stack(w, h), weights)
        return jax.tree.map(lambda total, term: total + term.astype(jnp.float32), so_far, back(by_y)[0]), None

    none_yet = {name: jnp.zeros(w.shape, jnp.float32) for name, w in weights.items()}
    by_weights, _ = lax.scan(take, none_yet, (x, dy))
    gradients = [by_weights[name].astype(jnp.bfloat16).astype(jnp.float32) for name in NAMES]
    new = [
        adamw(w.astype(jnp.float32), m, v, g)
        for w, m, v, g in zip((w_gate, w_up, w_down), (m_w_gate, m_w_up, m_w_down), (v_w_gate, v_w_up, v_w_down), gradients, strict=True)
    ]
    return tuple(one[which] for which in range(3) for one in new)
```

```python
import functools
import math

import jax
import jax.numpy as jnp
from jax import lax
from jax.experimental import pallas as pl
from jax.experimental.pallas import tpu as pltpu
from jax.sharding import PartitionSpec as P

BF16, F32 = jnp.bfloat16, jnp.float32
TILE = 256
LANES = 128
ROWS = 512
VMEM_LIMIT = 60 * 1024 * 1024


def dot(a, b, contract=((1,), (0,))):
    return lax.dot_general(a, b, (contract, ((), ())), preferred_element_type=F32)


def dot_t(a, b):
    return dot(a, b, ((1,), (1,)))


def scale_of(wide):
    return lax.rsqrt(jnp.mean(wide * wide, -1, keepdims=True) + 1e-6)


def sigmoid(x):
    return 0.5 * jnp.tanh(0.5 * x) + 0.5


def params(limit=VMEM_LIMIT):
    return pltpu.CompilerParams(vmem_limit_bytes=limit)


def whole(shape, layer=None):
    if layer is None:
        return pl.BlockSpec(shape, lambda *_: (0,) * len(shape), pipeline_mode=pl.Buffered(1))
    return pl.BlockSpec((None, *shape), lambda *_: (layer,) + (0,) * len(shape), pipeline_mode=pl.Buffered(1))


def cuts(total, size):
    return [(at, min(size, total - at)) for at in range(0, total, size)]


def forward_kernel(h_ref, dy_ref, wg_ref, wu_ref, wd_ref, gate_ref, up_ref, at_ref, h1_ref, a1_ref, a1t_ref, dyt_ref, hid_ref):
    h = h_ref[...].astype(F32)
    a = (h * scale_of(h)).astype(BF16)
    at_ref[...] = a.T
    dyt_ref[...] = dy_ref[...].T
    for at, n in cuts(wg_ref.shape[1], 1280):
        gate = dot(a, wg_ref[:, at : at + n])
        up = dot(a, wu_ref[:, at : at + n])
        gate_ref[:, at : at + n] = gate
        up_ref[:, at : at + n] = up
        hid_ref[:, at : at + n] = (gate * sigmoid(gate) * up).astype(BF16)
    z = dot(hid_ref[...], wd_ref[...]).astype(BF16)
    h1 = (h + z.astype(F32)).astype(BF16)
    h1_ref[...] = h1
    h1 = h1.astype(F32)
    a1 = (h1 * scale_of(h1)).astype(BF16)
    a1_ref[...] = a1
    a1t_ref[...] = a1.T


def forward(h, dy, wg, wu, wd, layer):
    t, d = h.shape
    f = wg.shape[2]
    rows = pl.BlockSpec((ROWS, d), lambda i: (i, 0))
    hidden = pl.BlockSpec((ROWS, f), lambda i: (i, 0))
    columns = pl.BlockSpec((d, ROWS), lambda i: (0, i))
    return pl.pallas_call(
        forward_kernel,
        grid=(t // ROWS,),
        in_specs=[rows, rows, whole((d, f), layer), whole((d, f), layer), whole((f, d), layer)],
        out_specs=[hidden, hidden, columns, rows, rows, columns, columns],
        out_shape=[
            jax.ShapeDtypeStruct((t, f), F32),
            jax.ShapeDtypeStruct((t, f), F32),
            jax.ShapeDtypeStruct((d, t), BF16),
            jax.ShapeDtypeStruct((t, d), BF16),
            jax.ShapeDtypeStruct((t, d), BF16),
            jax.ShapeDtypeStruct((d, t), BF16),
            jax.ShapeDtypeStruct((d, t), BF16),
        ],
        scratch_shapes=[pltpu.VMEM((ROWS, f), BF16)],
        compiler_params=params(),
        cost_estimate=pl.CostEstimate(flops=6 * t * d * f, bytes_accessed=8 * t * f, transcendentals=t * f),
        name="forward",
    )(h, dy, wg, wu, wd)


def hidden_gradients(gate, up, dhid):
    dhid = dhid.astype(BF16).astype(F32)
    s = sigmoid(gate)
    silu = gate * s
    hid = (silu * up).astype(BF16)
    dup = (dhid * silu).astype(BF16)
    dgate = (dhid * up * (s + silu * (1.0 - s))).astype(BF16)
    return hid, dgate, dup


def store_gradients(g_ref, at_ref, dyt_ref, hid_ref, dgate_ref, dup_ref):
    d = at_ref.shape[0]
    for i, (left, right) in enumerate(((at_ref, dgate_ref), (at_ref, dup_ref), (dyt_ref, hid_ref))):
        g = dot(left[...], right[...]).astype(BF16)
        for k in range(TILE // LANES):
            g_ref[(3 * k + i) * d : (3 * k + i + 1) * d, :] = g[:, k * LANES : (k + 1) * LANES]


def last_kernel(a_ref, at_ref, dy_ref, dyt_ref, wg_ref, wu_ref, wd_ref, g_ref, dgate_ref, dup_ref, hid_ref):
    for at, n in cuts(a_ref.shape[0], ROWS):
        here = slice(at, at + n)
        gate = dot(a_ref[here, :], wg_ref[...])
        up = dot(a_ref[here, :], wu_ref[...])
        dhid = dot_t(dy_ref[here, :], wd_ref[...])
        hid_ref[here, :], dgate_ref[here, :], dup_ref[here, :] = hidden_gradients(gate, up, dhid)
    store_gradients(g_ref, at_ref, dyt_ref, hid_ref, dgate_ref, dup_ref)


def flat(d, rows):
    return pl.BlockSpec((3 * d * (TILE // LANES), LANES), lambda j: (j, 0)), jax.ShapeDtypeStruct((rows, LANES), BF16)


def last_backward(a, at, dy, dyt, wg, wu, wd, layer, rows):
    t, d = a.shape
    f = wg.shape[2]
    columns = pl.BlockSpec((None, d, TILE), lambda j: (layer, 0, j))
    out = pl.BlockSpec((t, TILE), lambda j: (0, j))
    spec, shape = flat(d, rows)
    return pl.pallas_call(
        last_kernel,
        grid=(pl.cdiv(f, TILE),),
        in_specs=[
            whole((t, d)),
            whole((d, t)),
            whole((t, d)),
            whole((d, t)),
            columns,
            columns,
            pl.BlockSpec((None, TILE, d), lambda j: (layer, j, 0)),
        ],
        out_specs=[spec, out, out],
        out_shape=[shape, jax.ShapeDtypeStruct((t, f), BF16), jax.ShapeDtypeStruct((t, f), BF16)],
        scratch_shapes=[pltpu.VMEM((t, TILE), BF16)],
        compiler_params=params(),
        cost_estimate=pl.CostEstimate(flops=12 * t * d * f, bytes_accessed=6 * t * f, transcendentals=t * f),
        name="last_backward",
    )(a, at, dy, dyt, wg, wu, wd)


def first_kernel(gate_ref, up_ref, at_ref, dy_ref, dyt_ref, wd_ref, g_ref, hid_ref, dgate_ref, dup_ref):
    for at, n in cuts(dy_ref.shape[0], ROWS):
        here = slice(at, at + n)
        dhid = dot_t(dy_ref[here, :], wd_ref[...])
        hid_ref[here, :], dgate_ref[here, :], dup_ref[here, :] = hidden_gradients(gate_ref[here, :], up_ref[here, :], dhid)
    store_gradients(g_ref, at_ref, dyt_ref, hid_ref, dgate_ref, dup_ref)


def first_backward(gate, up, at, dy, dyt, wd, layer, rows):
    t, d = dy.shape
    f = wd.shape[1]
    hidden = pl.BlockSpec((t, TILE), lambda j: (0, j))
    spec, shape = flat(d, rows)
    return pl.pallas_call(
        first_kernel,
        grid=(pl.cdiv(f, TILE),),
        in_specs=[hidden, hidden, whole((d, t)), whole((t, d)), whole((d, t)), pl.BlockSpec((None, TILE, d), lambda j: (layer, j, 0))],
        out_specs=spec,
        out_shape=shape,
        scratch_shapes=[pltpu.VMEM((t, TILE), BF16)] * 3,
        compiler_params=params(),
        cost_estimate=pl.CostEstimate(flops=8 * t * d * f, bytes_accessed=8 * t * f, transcendentals=t * f),
        name="first_backward",
    )(gate, up, at, dy, dyt, wd)


def input_kernel(h_ref, dy_ref, wg_ref, wu_ref, dgate_ref, dup_ref, dh_ref, dht_ref):
    da = dot_t(dgate_ref[...], wg_ref[...]) + dot_t(dup_ref[...], wu_ref[...])
    da = da.astype(BF16).astype(F32)
    h = h_ref[...].astype(F32)
    scale = scale_of(h)
    along = jnp.sum(da * h, -1, keepdims=True)
    by_norm = da * scale - h * (scale * scale * scale * along / h.shape[1])
    dh = (dy_ref[...].astype(F32) + by_norm.astype(BF16).astype(F32)).astype(BF16)
    dh_ref[...] = dh
    dht_ref[...] = dh.T


def input_gradient(h, dy, wg, wu, dgate, dup, layer):
    t, d = h.shape
    f = wg.shape[2]
    rows = pl.BlockSpec((ROWS, d), lambda i: (i, 0))
    hidden = pl.BlockSpec((ROWS, f), lambda i: (i, 0))
    return pl.pallas_call(
        input_kernel,
        grid=(t // ROWS,),
        in_specs=[rows, rows, whole((d, f), layer), whole((d, f), layer), hidden, hidden],
        out_specs=[rows, pl.BlockSpec((d, ROWS), lambda i: (0, i))],
        out_shape=[jax.ShapeDtypeStruct((t, d), BF16), jax.ShapeDtypeStruct((d, t), BF16)],
        compiler_params=params(),
        cost_estimate=pl.CostEstimate(flops=4 * t * d * f, bytes_accessed=4 * t * f, transcendentals=0),
        name="input_gradient",
    )(h, dy, wg, wu, dgate, dup)


def where(side):
    me = lax.axis_index("dp")
    core = me % 2
    return core, me // 2 // side, me // 2 % side


def device(side, core, x, y, k, w):
    u, v = x * (1 - core) + y * core, y * (1 - core) + x * core
    u, v = (u + k) % side, (v + w) % side
    return ((u * (1 - core) + v * core) * side + v * (1 - core) + u * core) * 2 + core


def add_into(out, rows, *refs):
    step = next(n for n in (64, 32, 16) if rows % n == 0)

    def body(i, _):
        here = pl.ds(pl.multiple_of(i * step, step), step)
        total = refs[0][here, :].astype(F32)
        for ref in refs[1:]:
            total = total + ref[here, :].astype(F32)
        out[here, :] = total.astype(out.dtype)
        return _

    lax.fori_loop(0, rows // step, body, 0)


def scatter_kernel(side, g_ref, out_ref, mine, theirs, relay, beside, stay, relay2, beside2, load_sem, pair_send, pair_recv, send, recv):
    core, x, y = where(side)
    n = out_ref.shape[0]
    half = n // 2
    partner = (x * side + y) * 2 + 1 - core
    right, left = device(side, core, x, y, 1, 0), device(side, core, x, y, side - 1, 0)
    ahead, behind = device(side, core, x, y, 0, 1), device(side, core, x, y, 0, side - 1)

    barrier = pltpu.get_barrier_semaphore()
    for other in (partner, right, left, ahead, behind):
        pl.semaphore_signal(barrier, inc=1, device_id={"dp": other}, device_id_type=pl.DeviceIdType.MESH)
    pl.semaphore_wait(barrier, 5)

    def remote(src, dst, send_sem, recv_sem, to):
        return pltpu.make_async_remote_copy(
            src_ref=src, dst_ref=dst, send_sem=send_sem, recv_sem=recv_sem, device_id={"dp": to}, device_id_type=pl.DeviceIdType.MESH
        )

    def segment(of, k, w):
        row = device(side, of, x, y, k, w) * n
        return g_ref.at[pl.ds(pl.multiple_of(row, n), n), :]

    def slot(k, w):
        return pl.ds((k * side + w) * n, n)

    order = [(k, w) for k in (2, 1, 3, 0) for w in range(side)]
    pair, load = {}, {}
    for k, w in order:
        i = k * side + w
        pair[k, w] = remote(segment(1 - core, k, w), theirs.at[slot(k, w), :], pair_send.at[i], pair_recv.at[i], partner)
        pair[k, w].start()
        load[k, w] = pltpu.make_async_copy(segment(core, k, w), mine.at[slot(k, w), :], load_sem.at[i])
        load[k, w].start()

    def here(k, w):
        load[k, w].wait()
        pair[k, w].wait_recv()

    def two(ref, k, w):
        return ref.at[pl.ds((k * side + w) * n, 2 * n), :]

    copies = []

    def go(i, src, dst, to):
        copies.append(remote(src, dst, send.at[i], recv.at[i], to))
        copies[-1].start()
        return copies[-1]

    def summed(k, w):
        for one in (w, w + 1):
            here(k, one)
        add_into(two(mine, k, w), 2 * n, two(mine, k, w), two(theirs, k, w))

    summed(2, 0)
    from_left = go(0, two(mine, 2, 0), relay.at[pl.ds(0, 2 * n), :], right)
    summed(2, 2)
    from_right = go(1, two(mine, 2, 2), relay.at[pl.ds(2 * n, 2 * n), :], left)
    summed(1, 2)
    by_left = [go(2, two(mine, 1, 2), two(beside, 0, 2), right)]
    summed(3, 0)
    by_right = [go(3, two(mine, 3, 0), two(beside, 1, 0), left)]
    for one in (0, 1):
        here(1, one)
    from_left.wait_recv()
    add_into(two(mine, 1, 0), 2 * n, two(mine, 1, 0), two(theirs, 1, 0), relay.at[pl.ds(0, 2 * n), :])
    by_left.append(go(4, two(mine, 1, 0), two(beside, 0, 0), right))
    for one in (2, 3):
        here(3, one)
    from_right.wait_recv()
    add_into(two(mine, 3, 2), 2 * n, two(mine, 3, 2), two(theirs, 3, 2), relay.at[pl.ds(2 * n, 2 * n), :])
    by_right.append(go(5, two(mine, 3, 2), two(beside, 1, 2), left))
    for one in range(side):
        here(0, one)
    for one in by_left + by_right:
        one.wait_recv()

    def own(w, out):
        at = slot(0, w)
        add_into(out, n, mine.at[at, :], theirs.at[at, :], beside.at[slot(0, w), :], beside.at[slot(1, w), :])

    def part(w, which):
        return mine.at[pl.ds(w * n + which * half, half), :]

    own(2, mine.at[slot(0, 2), :])
    from_left = go(6, part(2, 0), relay2.at[pl.ds(0, half), :], ahead)
    from_right = go(7, part(2, 1), relay2.at[pl.ds(half, half), :], behind)
    own(1, mine.at[slot(0, 1), :])
    by_left = [go(8, part(1, 1), beside2.at[pl.ds(half, half), :], ahead)]
    own(3, mine.at[slot(0, 3), :])
    by_right = [go(9, part(3, 0), beside2.at[pl.ds(n, half), :], behind)]
    from_left.wait_recv()
    add_into(part(1, 0), half, part(1, 0), relay2.at[pl.ds(0, half), :])
    by_left.append(go(10, part(1, 0), beside2.at[pl.ds(0, half), :], ahead))
    from_right.wait_recv()
    add_into(part(3, 1), half, part(3, 1), relay2.at[pl.ds(half, half), :])
    by_right.append(go(11, part(3, 1), beside2.at[pl.ds(n + half, half), :], behind))
    own(0, stay)
    for one in by_left + by_right:
        one.wait_recv()
    add_into(out_ref, n, stay, beside2.at[pl.ds(0, n), :], beside2.at[pl.ds(n, n), :])
    for one in list(pair.values()) + copies:
        one.wait_send()


def scatter(g, side, collective_id):
    n = g.shape[0] // (2 * side * side)
    return pl.pallas_call(
        functools.partial(scatter_kernel, side),
        in_specs=[pl.BlockSpec(memory_space=pl.ANY)],
        out_specs=pl.BlockSpec(memory_space=pltpu.VMEM),
        out_shape=jax.ShapeDtypeStruct((n, LANES), BF16),
        scratch_shapes=[
            pltpu.VMEM((side * side * n, LANES), BF16),
            pltpu.VMEM((side * side * n, LANES), BF16),
            pltpu.VMEM((side * n, LANES), BF16),
            pltpu.VMEM((2 * side * n, LANES), BF16),
            pltpu.VMEM((n, LANES), F32),
            pltpu.VMEM((n, LANES), BF16),
            pltpu.VMEM((2 * n, LANES), BF16),
            pltpu.SemaphoreType.DMA((side * side,)),
            pltpu.SemaphoreType.DMA((side * side,)),
            pltpu.SemaphoreType.DMA((side * side,)),
            pltpu.SemaphoreType.DMA((12,)),
            pltpu.SemaphoreType.DMA((12,)),
        ],
        compiler_params=pltpu.CompilerParams(collective_id=collective_id, has_side_effects=True, vmem_limit_bytes=VMEM_LIMIT),
        cost_estimate=pl.CostEstimate(flops=40_000_000_000, bytes_accessed=2 * g.size, transcendentals=0),
        name="scatter",
    )(g)


def adamw(w, m, v, g):
    m = 0.9 * m + 0.1 * g
    v = 0.95 * v + 0.05 * g * g
    step = m * lax.rsqrt(v + 1e-8) + 0.1 * w
    return (w - 0.02 * step).astype(BF16), m, v


def adamw_kernel(given, g_ref, *refs):
    ins, outs = refs[:9], refs[9 + given :]
    d = g_ref.shape[0] // 3
    for i in range(3):
        g = g_ref[i * d : (i + 1) * d, :]
        g = (g.T if i == 2 else g).astype(F32)
        outs[i][...], outs[3 + i][...], outs[6 + i][...] = adamw(ins[i][...].astype(F32), ins[3 + i][...], ins[6 + i][...], g)


def update(g, arrays, so_far, layer):
    _, d, f = arrays[0].shape
    wide = pl.BlockSpec((None, d, LANES), lambda j: (layer, 0, j))
    tall = pl.BlockSpec((None, LANES, d), lambda j: (layer, j, 0))
    specs = [wide, wide, tall] * 3
    given = 0 if so_far is None else 9
    return pl.pallas_call(
        functools.partial(adamw_kernel, given),
        grid=(f // LANES,),
        in_specs=[pl.BlockSpec((3 * d, LANES), lambda j: (j, 0))] + specs + [pl.BlockSpec(memory_space=pl.ANY)] * given,
        out_specs=specs,
        out_shape=[jax.ShapeDtypeStruct(one.shape, one.dtype) for one in arrays],
        input_output_aliases={10 + i: i for i in range(given)},
        compiler_params=params(),
        cost_estimate=pl.CostEstimate(flops=36 * d * f, bytes_accessed=66 * d * f, transcendentals=3 * d * f),
        name="adamw",
    )(g, *arrays, *(so_far or ()))


def solution(mesh):
    size = mesh.shape["dp"]
    side = math.isqrt(size // 2)

    def step(x, dy, *arrays):
        wg, wu, wd = arrays[:3]
        layers, d, f = wg.shape
        assert layers == 2 and side == 4 and 2 * side * side == size and f % LANES == 0
        dy = dy[0]
        rows = pl.cdiv(3 * d * f // LANES, 32 * size) * 32 * size
        gate, up, at0, h1, a1, a1t, dyt = forward(x[0], dy, wg, wu, wd, 0)
        g, dgate, dup = last_backward(a1, a1t, dy, dyt, wg, wu, wd, 1, rows)
        late = lax.psum(g, "dp")
        dh, dht = input_gradient(h1, dy, wg, wu, dgate, dup, 1)
        g = first_backward(gate, up, at0, dh, dht, wd, 0, rows)
        early = scatter(g, side, 0)
        late, early = lax.optimization_barrier((late, early))
        early = lax.all_gather(early, "dp", axis=0, tiled=True)
        new = update(late, arrays, None, 1)
        return tuple(update(early, arrays, new, 0))

    return jax.shard_map(
        step,
        mesh=mesh,
        in_specs=(P(("rep", "dp"), None, None),) * 2 + (P(None, None, None),) * 9,
        out_specs=(P("rep", None, None),) * 9,
        check_vma=False,
    )
```
